128 devices in a mesh: group: 4 (over x, y), blk: 32 (over z, core).
Axes of the slice: x: 2, y: 2, z: 16, core: 2. Of those that a mesh axis runs over, the one named last changes fastest.
The devices are a block of a 8x8x16 slice.
Arguments:
- depth_logits: float32 [128, 112, 32, 128], P(('group', 'blk')), parts along dimension 0, may hold values from -18 to 300
- context: bfloat16 [128, 80, 32, 128], P(('group', 'blk')), parts along dimension 0, may hold values from -6 to 6
- lidar_bins: int32 [128, 32, 128], P(('group', 'blk')), parts along dimension 0, may hold values from -1 to 111, as said below
- az_map: int32 [8, 128], replicated, may hold values from 0 to 255, as said below
- rng_map: int32 [8, 112], replicated, may hold values from 0 to 511, as said below
- conv1_weight: bfloat16 [3, 3, 80, 256], replicated, may hold values from -0.21875 to 0.21875
- conv2_weight: bfloat16 [3, 3, 256, 256], replicated, may hold values from -0.125 to 0.125
- out_grad: bfloat16 [1024, 512, 256], P(('group', 'blk')), parts along dimension 0, may hold values from -6 to 6
Outputs:
- logit_grad: float32 [128, 112, 32, 128], P(('group', 'blk')), parts along dimension 0
- context_grad: bfloat16 [128, 80, 32, 128], P(('group', 'blk')), parts along dimension 0
- conv1_grad: float32 [12, 3, 80, 256], P('group'), parts along dimension 0
- conv2_grad: float32 [12, 3, 256, 256], P('group'), parts along dimension 0
The draws below stay inside these ranges and needn't reach their ends.
There are 4 independent parts, one for each index of `group`. The reference program is written for one: setup_inputs(seed, part) draws one part's arguments, and reference() takes and returns one part's arrays. A program takes and returns all parts, laid end to end along the dimension named above; an argument that names none is the same for every part. Nothing has to cross between parts.
Inputs may be any that keep to these rules, and one draw needn't show every extreme that they name: `lidar_bins`: -1 marks a pixel without a LiDAR return. `az_map`: with S = 32, the columns of camera c, in order and never going back, run through the azimuth cells (c * S - S // 4 + t) mod 256 for t = 0 to 3 * S // 2 - 1, each such cell taking two or three columns. `rng_map`: for each camera the range cell rises strictly with the depth bin.
All inputs are finite; a program needn't handle non-finite values.
Results may differ from the reference program's by a relative error of at most 0.024.
Values may be sent and summed in bfloat16 or wider, within the bound.
A program may use at most 128 MiB of HBM per device.

```python
import jax
import jax.numpy as jnp
from jax import lax

BINS = 112
CH = 80
HID = 256
CAMS = 8
RG = 512
ROWS_DEV = 32
VIEWS = 32
AZ = 256
COLS = 128


def draw_depth_logits(key, part):
    shape = (VIEWS, BINS, ROWS_DEV, COLS)
    keys = jax.random.split(key, 1)
    return jnp.clip(3.0 * jax.random.normal(keys[0], shape, jnp.float32), -18.0, 18.0)


def draw_lidar_bins(key, part):
    keys = jax.random.split(key, 2)
    shape = (VIEWS, ROWS_DEV, COLS)
    has_return = jax.random.randint(keys[0], shape, 0, 3) == 0
    chosen = jax.random.randint(keys[1], shape, 0, BINS)
    return jnp.where(has_return, chosen, -1).astype(jnp.int32)


def draw_az_map(key, part):
    span = AZ // CAMS
    field_cells = 3 * span // 2
    keys = jax.random.split(key, CAMS)

    def one_camera(camera_key, camera):
        order = jax.random.permutation(camera_key, field_cells)
        counts = jnp.where(order < span // 2, 2, 3).astype(jnp.int32)
        ends = jnp.cumsum(counts)
        column_index = jnp.arange(COLS, dtype=jnp.int32)
        local = jnp.sum((ends[None, :] <= column_index[:, None]).astype(jnp.int32), axis=1)
        return (camera * span - span // 4 + local) % AZ
    return jax.vmap(one_camera)(keys, jnp.arange(CAMS, dtype=jnp.int32)).astype(jnp.int32)


def draw_rng_map(key, part):
    keys = jax.random.split(key, CAMS)

    def one_camera(camera_key):
        return jnp.sort(jax.random.permutation(camera_key, RG)[:BINS])
    return jax.vmap(one_camera)(keys).astype(jnp.int32)


def block_levels(rng, extent, cuts, low, top_value):
    def one(dim, parts):
        steps = jax.random.uniform(jax.random.fold_in(jax.random.fold_in(rng, 6), dim), (parts,), jnp.float32, low / len(cuts), top_value / len(cuts))
        return jnp.repeat(jnp.exp(steps), extent[dim] // parts).reshape((-1,) + (1,) * (len(extent) - dim - 1))

    loudness = one(*cuts[0])
    for cut in cuts[1:]:
        loudness = loudness * one(*cut)
    return loudness


def noise(stream_key, extent, scale, limit, cuts=(), kind=jnp.bfloat16):
    level = block_levels(stream_key, extent, cuts, -0.22, 0.18) if cuts else 1.0
    values = jax.random.normal(stream_key, extent, jnp.float32) * scale * level
    return jnp.minimum(jnp.maximum(values, -limit), limit).astype(kind)


def setup_inputs(seed: int = 0, part: int = 0) -> dict:
    arg_keys = jax.random.split(jax.random.key(seed), 9)
    part_keys = jax.random.split(jax.random.fold_in(arg_keys[8], part), 9)
    return {
        "depth_logits": draw_depth_logits(jax.random.fold_in(jax.random.fold_in(arg_keys[8], part), 71), part),
        "context": noise(part_keys[1], (VIEWS, CH, ROWS_DEV, COLS), 1.0, 6.0, ((0, 32),)),
        "lidar_bins": draw_lidar_bins(jax.random.fold_in(jax.random.fold_in(arg_keys[8], part), 71), part),
        "az_map": draw_az_map(jax.random.fold_in(arg_keys[8], 71), part),
        "rng_map": draw_rng_map(jax.random.fold_in(arg_keys[8], 71), part),
        "conv1_weight": noise(arg_keys[5], (3, 3, CH, HID), (9 * CH) ** -0.5, 0.21875),
        "conv2_weight": noise(arg_keys[6], (3, 3, HID, HID), (9 * HID) ** -0.5, 0.125),
        "out_grad": noise(part_keys[7], (AZ, RG, HID), 1.0, 6.0, ((0, 32),)),
    }


DEPTH_WEIGHT = 3.0
precise = lax.Precision.HIGHEST

def shifted(field, tap_row, tap_col):
    rolled = jnp.roll(field, 1 - tap_row, axis=0)
    padded = jnp.pad(rolled, ((0, 0), (1, 1), (0, 0)))
    return padded[:, tap_col:tap_col + field.shape[1]]

def convolve(field, weight):
    running = jnp.zeros(field.shape[:2] + (weight.shape[3],), jnp.float32)
    for tap_row in range(3):
        for tap_col in range(3):
            running = running + jnp.einsum('arc,co->aro', shifted(field, tap_row, tap_col).astype(jnp.float32), weight[tap_row, tap_col].astype(jnp.float32), precision=precise)
    return running

def input_grad(grad_field, weight):
    running = jnp.zeros(grad_field.shape[:2] + (weight.shape[2],), jnp.float32)
    for tap_row in range(3):
        for tap_col in range(3):
            running = running + jnp.einsum('aro,co->arc', shifted(grad_field, 2 - tap_row, 2 - tap_col).astype(jnp.float32), weight[tap_row, tap_col].astype(jnp.float32), precision=precise)
    return running

def weight_grad(field, grad_field):
    outer_rows = []
    for tap_row in range(3):
        outer_cols = []
        for tap_col in range(3):
            outer_cols.append(jnp.einsum('arc,aro->co', shifted(field, tap_row, tap_col).astype(jnp.float32), grad_field.astype(jnp.float32), precision=precise))
        outer_rows.append(jnp.stack(outer_cols))
    return jnp.stack(outer_rows)

def silu_slope(value):
    logistic = jax.nn.sigmoid(value)
    return logistic * (1.0 + value * (1.0 - logistic))

def reference(depth_logits, context, lidar_bins, az_map, rng_map, conv1_weight, conv2_weight, out_grad):
    view_count = depth_logits.shape[0]
    band_count = view_count // CAMS
    az_total = out_grad.shape[0]
    probs = jax.nn.softmax(depth_logits, axis=1)
    probs_low = probs.astype(jnp.bfloat16)
    wedge = jnp.einsum('vbrc,vhrc->vcbh', probs_low.astype(jnp.float32), context.astype(jnp.float32), precision=precise).astype(jnp.bfloat16)

    def place(running, view_index):
        camera = view_index // band_count
        sector_piece = jnp.zeros((az_total, BINS, CH), jnp.float32).at[az_map[camera]].add(wedge[view_index].astype(jnp.float32))
        sector_piece = lax.optimization_barrier(sector_piece.astype(jnp.bfloat16)).astype(jnp.float32)
        running = running.at[:, rng_map[camera], :].add(sector_piece)
        return (running, None)
    bev, _ = lax.scan(place, jnp.zeros((az_total, RG, CH), jnp.float32), jnp.arange(view_count, dtype=jnp.int32))
    bev_low = bev.astype(jnp.bfloat16)
    hidden_pre = convolve(bev_low, conv1_weight)
    activated = jax.nn.silu(hidden_pre).astype(jnp.bfloat16)
    conv2_grad = weight_grad(activated, out_grad)
    act_grad = input_grad(out_grad, conv2_weight)
    pre_grad = (act_grad * silu_slope(hidden_pre)).astype(jnp.bfloat16)
    conv1_grad = weight_grad(bev_low, pre_grad)
    bev_grad = input_grad(pre_grad, conv1_weight).astype(jnp.bfloat16)

    def view_grads(view_index):
        camera = view_index // band_count
        wedge_grad = bev_grad[az_map[camera]][:, rng_map[camera], :].astype(jnp.float32)
        prob_grad = jnp.einsum('cbh,hrc->brc', wedge_grad, context[view_index].astype(jnp.float32), precision=precise)
        ctx_grad = jnp.einsum('cbh,brc->hrc', wedge_grad, probs_low[view_index].astype(jnp.float32), precision=precise).astype(jnp.bfloat16)
        depth_prob = probs[view_index]
        expected = lax.optimization_barrier(jnp.sum(depth_prob * prob_grad, axis=0, keepdims=True))
        lidar_row = lidar_bins[view_index]
        onehot = (jnp.arange(BINS, dtype=jnp.int32)[:, None, None] == lidar_row[None]).astype(jnp.float32)
        has_return = (lidar_row >= 0).astype(jnp.float32)[None]
        grad_logit = depth_prob * (prob_grad - expected) + DEPTH_WEIGHT * (has_return * depth_prob - onehot)
        return (grad_logit, ctx_grad)
    logit_grad, context_grad = lax.map(view_grads, jnp.arange(view_count, dtype=jnp.int32))
    return (logit_grad, context_grad, conv1_grad, conv2_grad)
```

```python
import jax
import jax.numpy as jnp
from jax import lax
from jax.experimental import pallas as pl
from jax.experimental.pallas import tpu as pltpu
from jax.sharding import PartitionSpec as P

DEPTH_WEIGHT = 3.0


def with_halo(cells, width):
    count = lax.axis_size("blk")
    head = cells[:width]
    tail = cells[cells.shape[0] - width :]
    return jnp.concatenate(
        [
            lax.ppermute(tail, "blk", [(i, (i + 1) % count) for i in range(count)]),
            cells,
            lax.ppermute(head, "blk", [((i + 1) % count, i) for i in range(count)]),
        ],
        axis=0,
    )


def silu_slope(value):
    logistic = jax.nn.sigmoid(value)
    return logistic * (1.0 + value * (1.0 - logistic))


def remote(src, dst, send_sem, recv_sem, target):
    return pltpu.make_async_remote_copy(
        src_ref=src,
        dst_ref=dst,
        send_sem=send_sem,
        recv_sem=recv_sem,
        device_id={"blk": target},
        device_id_type=pl.DeviceIdType.MESH,
    )


def greet(semaphore, target):
    pl.semaphore_signal(
        semaphore,
        inc=1,
        device_id={"blk": target},
        device_id_type=pl.DeviceIdType.MESH,
    )


def scatter_kernel(blocks, bands, pieces, sums, slots, send_sems, recv_sems):
    me = lax.axis_index("blk")
    band = me % bands
    first = me - band
    before = (first + blocks - bands) % blocks
    after = (first + bands) % blocks
    barrier = pltpu.get_barrier_semaphore()
    for other in range(bands):
        @pl.when(band != other)
        def _():
            greet(barrier, first + other)

        @pl.when(band == 0)
        def _():
            greet(barrier, before + other)

        @pl.when(band == bands - 1)
        def _():
            greet(barrier, after + other)
    pl.semaphore_wait(barrier, bands + 1)

    def outgoing(part):
        near = 1 <= part <= bands
        slot = band if near else bands + band
        target = (first + blocks - 1 + part) % blocks
        return remote(
            pieces.at[part], slots.at[slot], send_sems.at[part], recv_sems.at[slot], target
        )

    def arriving(slot):
        return remote(pieces.at[0], slots.at[slot], send_sems.at[0], recv_sems.at[slot], first)

    for part in (0, bands + 1):
        outgoing(part).start()
    for part in range(1, bands + 1):
        @pl.when(band != part - 1)
        def _():
            outgoing(part).start()
    slots[pl.ds(band, 1)] = pieces[pl.ds(band + 1, 1)]
    for slot in range(bands):
        @pl.when(band != slot)
        def _():
            arriving(slot).wait_recv()
    total = slots[0].astype(jnp.float32)
    for slot in range(1, bands):
        total = total + slots[slot].astype(jnp.float32)
    sums[0] = total.astype(sums.dtype)
    edge = jnp.logical_or(band == 0, band == bands - 1)

    @pl.when(edge)
    def _():
        for slot in range(bands, 2 * bands):
            arriving(slot).wait_recv()
        side = slots[bands].astype(jnp.float32)
        for slot in range(bands + 1, 2 * bands):
            side = side + slots[slot].astype(jnp.float32)
        sums[1] = side.astype(sums.dtype)

    @pl.when(jnp.logical_not(edge))
    def _():
        sums[1] = jnp.zeros(sums.shape[1:], sums.dtype)

    for part in (0, bands + 1):
        outgoing(part).wait_send()
    for part in range(1, bands + 1):
        @pl.when(band != part - 1)
        def _():
            outgoing(part).wait_send()


def reply_kernel(blocks, bands, replies, gathered, send_sems, recv_sems):
    me = lax.axis_index("blk")
    band = me % bands
    first = me - band
    before = (first + blocks - bands) % blocks
    after = (first + bands) % blocks
    edge = jnp.logical_or(band == 0, band == bands - 1)
    barrier = pltpu.get_barrier_semaphore()
    greet(barrier, (first + blocks - 1) % blocks)
    greet(barrier, after)
    for other in range(bands):
        @pl.when(band != other)
        def _():
            greet(barrier, first + other)

    @pl.when(edge)
    def _():
        pl.semaphore_wait(barrier, 2 * bands - 1)

    @pl.when(jnp.logical_not(edge))
    def _():
        pl.semaphore_wait(barrier, bands - 1)

    def near(other):
        return remote(
            replies.at[0],
            gathered.at[band + 1],
            send_sems.at[other],
            recv_sems.at[band + 1],
            first + other,
        )

    def far_after(other):
        return remote(
            replies.at[1],
            gathered.at[0],
            send_sems.at[bands + other],
            recv_sems.at[0],
            after + other,
        )

    def far_before(other):
        return remote(
            replies.at[1],
            gathered.at[bands + 1],
            send_sems.at[bands + other],
            recv_sems.at[bands + 1],
            before + other,
        )

    def arriving(part):
        return remote(
            replies.at[0], gathered.at[part], send_sems.at[0], recv_sems.at[part], first
        )

    for other in range(bands):
        @pl.when(band == 0)
        def _():
            far_before(other).start()

        @pl.when(band == bands - 1)
        def _():
            far_after(other).start()

        @pl.when(band != other)
        def _():
            near(other).start()
    gathered[pl.ds(band + 1, 1)] = replies[pl.ds(0, 1)]
    for part in (0, bands + 1):
        arriving(part).wait_recv()
    for other in range(bands):
        @pl.when(band != other)
        def _():
            arriving(other + 1).wait_recv()
            near(other).wait_send()

        @pl.when(band == 0)
        def _():
            far_before(other).wait_send()

        @pl.when(band == bands - 1)
        def _():
            far_after(other).wait_send()


def context_part(wide, probs, grad, start, count):
    channels = grad.shape[0]

    def add(depth, sums):
        weight = probs[pl.ds(depth, 1)][0]
        return tuple(
            held + wide[pl.ds(depth * channels + start + step, 1), :] * weight
            for step, held in enumerate(sums)
        )

    zero = jnp.zeros(probs.shape[1:], jnp.float32)
    sums = lax.fori_loop(0, probs.shape[0], add, (zero,) * count, unroll=2)
    for step, held in enumerate(sums):
        grad[start + step] = held.astype(grad.dtype)


def prob_part(wide, features, probs, grad, mean, start, count):
    channels = features.shape[0]

    def add(channel, sums):
        feature = features[pl.ds(channel, 1)][0]
        return tuple(
            held + wide[pl.ds((start + step) * channels + channel, 1), :] * feature
            for step, held in enumerate(sums)
        )

    zero = jnp.zeros(probs.shape[1:], jnp.float32)
    sums = lax.fori_loop(0, channels, add, (zero,) * count, unroll=2)
    total = mean[...]
    for step, held in enumerate(sums):
        grad[start + step] = held
        total = total + probs[start + step] * held
    mean[...] = total


def logit_part(probs, lidar, grad, mean):
    named = lidar[...]
    kept = (named >= 0).astype(jnp.float32)
    expected = mean[...]

    def one(depth, carry):
        prob = probs[pl.ds(depth, 1)][0]
        hit = (named == depth).astype(jnp.float32)
        value = prob * (grad[pl.ds(depth, 1)][0] - expected) + DEPTH_WEIGHT * (
            kept * prob - hit
        )
        grad[pl.ds(depth, 1)] = value[None]
        return carry

    lax.fori_loop(0, probs.shape[0], one, 0, unroll=2)


def sum_kernel(
    chips, terms, wide, probs, context, lidar, out, logit_grad, context_grad,
    features, mean, pair, local, stage_r, stage_l, land_r, land_l,
    pair_sems, ring_r, ring_l, pass_r, pass_l,
):
    me = lax.axis_index("blk")
    core = me % 2
    chip = me // 2
    blocks = 2 * chips
    partner = me + 1 - 2 * core
    right = (me + 2) % blocks
    left = (me + blocks - 2) % blocks
    rights = chips // 2
    lefts = chips - 1 - rights
    barrier = pltpu.get_barrier_semaphore()
    for other in (partner, right, left):
        greet(barrier, other)
    pl.semaphore_wait(barrier, 3)
    swap = remote(terms.at[1 - core], pair, pair_sems.at[0], pair_sems.at[1], partner)
    swap.start()
    features[...] = context[...].astype(jnp.float32)
    mean[...] = jnp.zeros_like(mean)
    parts = 2 * rights
    depths = probs.shape[0] // parts
    widths = context.shape[0] // parts
    swap.wait_recv()
    local[...] = (
        terms[pl.ds(core, 1)][0].astype(jnp.float32) + pair[...].astype(jnp.float32)
    )
    moves_r = []
    moves_l = []
    for step in range(rights):
        chunk = (chip + rights - step) % chips
        value = local[pl.ds(chunk, 1)][0]
        if step:
            moves_r[-1].wait_recv()
            value = value + land_r[step - 1].astype(jnp.float32)
        stage_r[step] = value.astype(stage_r.dtype)
        move = remote(
            stage_r.at[step], land_r.at[step], ring_r.at[0, step], ring_r.at[1, step], right
        )
        move.start()
        moves_r.append(move)
        if step < lefts:
            chunk = (chip + chips - lefts + step) % chips
            value = local[pl.ds(chunk, 1)][0]
            if step:
                moves_l[-1].wait_recv()
                value = value + land_l[step - 1].astype(jnp.float32)
            stage_l[step] = value.astype(stage_l.dtype)
            move = remote(
                stage_l.at[step], land_l.at[step], ring_l.at[0, step], ring_l.at[1, step], left
            )
            move.start()
            moves_l.append(move)
        for part in (2 * step, 2 * step + 1):
            context_part(wide, probs, context_grad, part * widths, widths)
    moves_l[-1].wait_recv()
    moves_r[-1].wait_recv()
    total = (
        local[pl.ds(chip, 1)][0]
        + land_r[rights - 1].astype(jnp.float32)
        + land_l[lefts - 1].astype(jnp.float32)
    )
    out[pl.ds(core, 1), pl.ds(chip, 1)] = total.astype(out.dtype)[None, None]

    def passing_r(step, origin):
        block = out.at[core, (origin + chips - step) % chips]
        return remote(block, block, pass_r.at[0, step], pass_r.at[1, step], right)

    def passing_l(step, origin):
        block = out.at[core, (origin + step) % chips]
        return remote(block, block, pass_l.at[0, step], pass_l.at[1, step], left)

    for step in range(rights):
        if step:
            passing_r(step - 1, chip + chips - 1).wait_recv()
        passing_r(step, chip).start()
        if step < lefts:
            if step:
                passing_l(step - 1, chip + 1).wait_recv()
            passing_l(step, chip).start()
        for part in (2 * step, 2 * step + 1):
            prob_part(wide, features, probs, logit_grad, mean, part * depths, depths)
    passing_l(lefts - 1, chip + 1).wait_recv()
    passing_r(rights - 1, chip + chips - 1).wait_recv()
    whole = remote(
        out.at[core], out.at[core], pair_sems.at[2], pair_sems.at[3], partner
    )
    whole.start()
    logit_part(probs, lidar, logit_grad, mean)
    remote(
        out.at[1 - core], out.at[1 - core], pair_sems.at[2], pair_sems.at[3], partner
    ).wait_recv()
    whole.wait_send()
    swap.wait_send()
    for move in moves_r + moves_l:
        move.wait_send()
    for step in range(rights):
        passing_r(step, chip).wait_send()
    for step in range(lefts):
        passing_l(step, chip).wait_send()


VMEM = pl.BlockSpec(memory_space=pltpu.VMEM)


def scatter_pieces(pieces, bands):
    blocks = lax.axis_size("blk")
    shape = pieces.shape[1:]

    def kernel(*refs):
        scatter_kernel(blocks, bands, *refs)

    return pl.pallas_call(
        kernel,
        out_shape=jax.ShapeDtypeStruct((2,) + shape, pieces.dtype),
        in_specs=[VMEM],
        out_specs=VMEM,
        scratch_shapes=[
            pltpu.VMEM((2 * bands,) + shape, pieces.dtype),
            pltpu.SemaphoreType.DMA((bands + 2,)),
            pltpu.SemaphoreType.DMA((2 * bands,)),
        ],
        compiler_params=pltpu.CompilerParams(collective_id=0, has_side_effects=True),
        name="scatter_pieces",
    )(pieces)


def gather_replies(replies, bands):
    blocks = lax.axis_size("blk")
    shape = replies.shape[1:]

    def kernel(*refs):
        reply_kernel(blocks, bands, *refs)

    return pl.pallas_call(
        kernel,
        out_shape=jax.ShapeDtypeStruct((bands + 2,) + shape, replies.dtype),
        in_specs=[VMEM],
        out_specs=VMEM,
        scratch_shapes=[
            pltpu.SemaphoreType.DMA((2 * bands,)),
            pltpu.SemaphoreType.DMA((bands + 2,)),
        ],
        compiler_params=pltpu.CompilerParams(collective_id=1, has_side_effects=True),
        name="gather_replies",
    )(replies)


def summed(terms, wide, probs, context, lidar):
    chips = terms.shape[1]
    rights = chips // 2
    lefts = chips - 1 - rights
    block = terms.shape[2:]
    kind = terms.dtype

    def kernel(*refs):
        sum_kernel(chips, *refs)

    return pl.pallas_call(
        kernel,
        out_shape=(
            jax.ShapeDtypeStruct(terms.shape, kind),
            jax.ShapeDtypeStruct(probs.shape, jnp.float32),
            jax.ShapeDtypeStruct(context.shape, context.dtype),
        ),
        in_specs=[VMEM] * 5,
        out_specs=(VMEM,) * 3,
        scratch_shapes=[
            pltpu.VMEM(context.shape, jnp.float32),
            pltpu.VMEM(probs.shape[1:], jnp.float32),
            pltpu.VMEM((chips,) + block, kind),
            pltpu.VMEM((chips,) + block, jnp.float32),
            pltpu.VMEM((rights,) + block, kind),
            pltpu.VMEM((lefts,) + block, kind),
            pltpu.VMEM((rights,) + block, kind),
            pltpu.VMEM((lefts,) + block, kind),
            pltpu.SemaphoreType.DMA((4,)),
            pltpu.SemaphoreType.DMA((2, rights)),
            pltpu.SemaphoreType.DMA((2, lefts)),
            pltpu.SemaphoreType.DMA((2, rights)),
            pltpu.SemaphoreType.DMA((2, lefts)),
        ],
        compiler_params=pltpu.CompilerParams(collective_id=2, has_side_effects=True),
        name="sum_gradients",
    )(terms, wide, probs, context, lidar)


def tripled(field):
    length = field.shape[1]
    padded = jnp.pad(field, ((0, 0), (1, 1), (0, 0)))
    return jnp.concatenate([padded[:, col : col + length] for col in range(3)], axis=2)


def conv_rows(triple, weight):
    height = triple.shape[0] - 2
    length = triple.shape[1]
    wide = jnp.concatenate([triple[row : row + height] for row in range(3)], axis=2)
    flat = wide.reshape(height * length, -1)
    return jnp.dot(
        flat, weight.reshape(-1, weight.shape[3]), preferred_element_type=jnp.float32
    ).reshape(height, length, weight.shape[3])


def weight_grad(triple, upstream):
    height, length, width = upstream.shape
    flat = upstream.reshape(height * length, width)
    rows = []
    for row in range(3):
        left = triple[row : row + height].reshape(height * length, -1)
        rows.append(
            lax.dot_general(
                left, flat, (((0,), (0,)), ((), ())), preferred_element_type=jnp.float32
            ).astype(jnp.bfloat16)
        )
    return jnp.concatenate(rows, axis=0)


def mirrored(weight):
    return jnp.flip(weight, (0, 1)).transpose(0, 1, 3, 2)


def shards(
    depth_logits, context, lidar_bins, az_map, rng_map, conv1_weight, conv2_weight, out_grad
):
    blocks = lax.axis_size("blk")
    position = lax.axis_index("blk")
    cameras = az_map.shape[0]
    bands = blocks // cameras
    sector, length, hidden_width = out_grad.shape
    bin_count = depth_logits.shape[1]
    channels = context.shape[1]
    columns = depth_logits.shape[3]
    camera = position // bands
    band = position % bands
    upstream_wide = with_halo(out_grad, 2)
    depth_prob = jax.nn.softmax(depth_logits[0], axis=0)
    probs_low = depth_prob.astype(jnp.bfloat16)
    view_context = context[0]
    wedge = jnp.einsum("brc,hrc->cbh", probs_low, view_context, preferred_element_type=jnp.float32)
    wedge = wedge.astype(jnp.bfloat16).reshape(columns, bin_count * channels)
    az_row = lax.dynamic_slice_in_dim(az_map, camera, 1, 0)[0]
    span = (bands + 2) * sector
    seen = ((camera * bands + blocks - 1) * sector + jnp.arange(span, dtype=jnp.int32)) % (
        blocks * sector
    )
    column_hot = (seen[:, None] == az_row[None, :]).astype(jnp.bfloat16)
    pieces = jnp.dot(column_hot, wedge, preferred_element_type=jnp.float32).astype(jnp.bfloat16)
    sums = scatter_pieces(pieces.reshape(bands + 2, sector, bin_count * channels), bands)
    neighbour = jnp.where(band == 0, camera + cameras - 1, camera + 1) % cameras
    cells = jnp.arange(length, dtype=jnp.int32)
    ranges = jnp.concatenate(
        [
            lax.dynamic_slice_in_dim(rng_map, camera, 1, 0),
            lax.dynamic_slice_in_dim(rng_map, neighbour, 1, 0),
        ],
        axis=0,
    )
    range_hot = (ranges[:, None, :] == cells[None, :, None]).astype(jnp.bfloat16)
    bev = jnp.einsum(
        "nrb,nabh->arh",
        range_hot,
        sums.reshape(2, sector, bin_count, channels),
        preferred_element_type=jnp.float32,
    ).astype(jnp.bfloat16)
    bev_triple = tripled(with_halo(bev, 2))
    hidden_pre = conv_rows(bev_triple, conv1_weight)
    activated = jax.nn.silu(hidden_pre).astype(jnp.bfloat16)
    conv2_grad = weight_grad(tripled(activated), out_grad)
    act_grad = conv_rows(tripled(upstream_wide), mirrored(conv2_weight))
    pre_grad = (act_grad * silu_slope(hidden_pre)).astype(jnp.bfloat16)
    conv1_grad = weight_grad(bev_triple[1:-1], pre_grad[1:-1])
    bev_grad = conv_rows(tripled(pre_grad), mirrored(conv1_weight)).astype(jnp.bfloat16)
    replies = jnp.einsum(
        "nrb,arh->nabh", range_hot, bev_grad, preferred_element_type=jnp.float32
    ).astype(jnp.bfloat16)
    gathered = gather_replies(replies.reshape(2, sector, bin_count * channels), bands)
    wide = lax.dot_general(
        gathered.reshape(span, bin_count * channels),
        column_hot,
        (((0,), (0,)), ((), ())),
        preferred_element_type=jnp.float32,
    )
    rows1 = conv1_grad.shape[0]
    rows2 = conv2_grad.shape[0]
    step = 16 * blocks
    padding = -(rows1 + rows2) % step
    terms = jnp.concatenate(
        [conv1_grad, conv2_grad, jnp.zeros((padding, hidden_width), jnp.bfloat16)], axis=0
    )
    terms, logit_grad, context_grad = summed(
        terms.reshape(2, blocks // 2, -1, hidden_width),
        wide,
        depth_prob,
        view_context,
        lidar_bins[0],
    )
    terms = terms.reshape(-1, hidden_width).astype(jnp.float32)
    return (
        logit_grad[None],
        context_grad[None],
        terms[:rows1].reshape(3, 3, channels, hidden_width),
        terms[rows1 : rows1 + rows2].reshape(3, 3, hidden_width, hidden_width),
    )


def solution(mesh):
    return jax.shard_map(
        shards,
        mesh=mesh,
        in_specs=(
            P(("group", "blk"), None, None, None),
            P(("group", "blk"), None, None, None),
            P(("group", "blk"), None, None),
            P(),
            P(),
            P(),
            P(),
            P(("group", "blk"), None, None),
        ),
        out_specs=(
            P(("group", "blk"), None, None, None),
            P(("group", "blk"), None, None, None),
            P("group", None, None, None),
            P("group", None, None, None),
        ),
        check_vma=False,
    )
```

```python
import jax
import jax.numpy as jnp
from jax import lax
from jax.experimental import pallas as pl
from jax.experimental.pallas import tpu as pltpu
from jax.sharding import PartitionSpec as P

DEPTH_WEIGHT = 3.0


def with_halo(cells, width):
    count = lax.axis_size("blk")
    head = cells[:width]
    tail = cells[cells.shape[0] - width :]
    return jnp.concatenate(
        [
            lax.ppermute(tail, "blk", [(i, (i + 1) % count) for i in range(count)]),
            cells,
            lax.ppermute(head, "blk", [((i + 1) % count, i) for i in range(count)]),
        ],
        axis=0,
    )


def silu_slope(value):
    logistic = jax.nn.sigmoid(value)
    return logistic * (1.0 + value * (1.0 - logistic))


def remote(src, dst, send_sem, recv_sem, target):
    return pltpu.make_async_remote_copy(
        src_ref=src,
        dst_ref=dst,
        send_sem=send_sem,
        recv_sem=recv_sem,
        device_id={"blk": target},
        device_id_type=pl.DeviceIdType.MESH,
    )


def greet(semaphore, target):
    pl.semaphore_signal(
        semaphore,
        inc=1,
        device_id={"blk": target},
        device_id_type=pl.DeviceIdType.MESH,
    )


def scatter_kernel(blocks, bands, pieces, sums, slots, send_sems, recv_sems):
    me = lax.axis_index("blk")
    band = me % bands
    first = me - band
    before = (first + blocks - bands) % blocks
    after = (first + bands) % blocks
    barrier = pltpu.get_barrier_semaphore()
    for other in range(bands):
        @pl.when(band != other)
        def _():
            greet(barrier, first + other)

        @pl.when(band == 0)
        def _():
            greet(barrier, before + other)

        @pl.when(band == bands - 1)
        def _():
            greet(barrier, after + other)
    pl.semaphore_wait(barrier, bands + 1)

    def outgoing(part):
        near = 1 <= part <= bands
        slot = band if near else bands + band
        target = (first + blocks - 1 + part) % blocks
        return remote(
            pieces.at[part], slots.at[slot], send_sems.at[part], recv_sems.at[slot], target
        )

    def arriving(slot):
        return remote(pieces.at[0], slots.at[slot], send_sems.at[0], recv_sems.at[slot], first)

    for part in (0, bands + 1):
        outgoing(part).start()
    for part in range(1, bands + 1):
        @pl.when(band != part - 1)
        def _():
            outgoing(part).start()
    slots[pl.ds(band, 1)] = pieces[pl.ds(band + 1, 1)]
    for slot in range(bands):
        @pl.when(band != slot)
        def _():
            arriving(slot).wait_recv()
    total = slots[0].astype(jnp.float32)
    for slot in range(1, bands):
        total = total + slots[slot].astype(jnp.float32)
    sums[0] = total.astype(sums.dtype)
    edge = jnp.logical_or(band == 0, band == bands - 1)

    @pl.when(edge)
    def _():
        for slot in range(bands, 2 * bands):
            arriving(slot).wait_recv()
        side = slots[bands].astype(jnp.float32)
        for slot in range(bands + 1, 2 * bands):
            side = side + slots[slot].astype(jnp.float32)
        sums[1] = side.astype(sums.dtype)

    @pl.when(jnp.logical_not(edge))
    def _():
        sums[1] = jnp.zeros(sums.shape[1:], sums.dtype)

    for part in (0, bands + 1):
        outgoing(part).wait_send()
    for part in range(1, bands + 1):
        @pl.when(band != part - 1)
        def _():
            outgoing(part).wait_send()


def reply_kernel(blocks, bands, replies, gathered, send_sems, recv_sems):
    me = lax.axis_index("blk")
    band = me % bands
    first = me - band
    before = (first + blocks - bands) % blocks
    after = (first + bands) % blocks
    edge = jnp.logical_or(band == 0, band == bands - 1)
    barrier = pltpu.get_barrier_semaphore()
    greet(barrier, (first + blocks - 1) % blocks)
    greet(barrier, after)
    for other in range(bands):
        @pl.when(band != other)
        def _():
            greet(barrier, first + other)

    @pl.when(edge)
    def _():
        pl.semaphore_wait(barrier, 2 * bands - 1)

    @pl.when(jnp.logical_not(edge))
    def _():
        pl.semaphore_wait(barrier, bands - 1)

    def near(other):
        return remote(
            replies.at[0],
            gathered.at[band + 1],
            send_sems.at[other],
            recv_sems.at[band + 1],
            first + other,
        )

    def far_after(other):
        return remote(
            replies.at[1],
            gathered.at[0],
            send_sems.at[bands + other],
            recv_sems.at[0],
            after + other,
        )

    def far_before(other):
        return remote(
            replies.at[1],
            gathered.at[bands + 1],
            send_sems.at[bands + other],
            recv_sems.at[bands + 1],
            before + other,
        )

    def arriving(part):
        return remote(
            replies.at[0], gathered.at[part], send_sems.at[0], recv_sems.at[part], first
        )

    for other in range(bands):
        @pl.when(band == 0)
        def _():
            far_before(other).start()

        @pl.when(band == bands - 1)
        def _():
            far_after(other).start()

        @pl.when(band != other)
        def _():
            near(other).start()
    gathered[pl.ds(band + 1, 1)] = replies[pl.ds(0, 1)]
    for part in (0, bands + 1):
        arriving(part).wait_recv()
    for other in range(bands):
        @pl.when(band != other)
        def _():
            arriving(other + 1).wait_recv()
            near(other).wait_send()

        @pl.when(band == 0)
        def _():
            far_before(other).wait_send()

        @pl.when(band == bands - 1)
        def _():
            far_after(other).wait_send()


def context_part(wide, probs, grad, start, count):
    channels = grad.shape[0]

    def add(depth, sums):
        weight = probs[pl.ds(depth, 1)][0]
        return tuple(
            held + wide[pl.ds(depth * channels + start + step, 1), :] * weight
            for step, held in enumerate(sums)
        )

    zero = jnp.zeros(probs.shape[1:], jnp.float32)
    sums = lax.fori_loop(0, probs.shape[0], add, (zero,) * count, unroll=2)
    for step, held in enumerate(sums):
        grad[start + step] = held.astype(grad.dtype)


def prob_part(wide, features, probs, grad, mean, start, count):
    channels = features.shape[0]

    def add(channel, sums):
        feature = features[pl.ds(channel, 1)][0]
        return tuple(
            held + wide[pl.ds((start + step) * channels + channel, 1), :] * feature
            for step, held in enumerate(sums)
        )

    zero = jnp.zeros(probs.shape[1:], jnp.float32)
    sums = lax.fori_loop(0, channels, add, (zero,) * count, unroll=2)
    total = mean[...]
    for step, held in enumerate(sums):
        grad[start + step] = held
        total = total + probs[start + step] * held
    mean[...] = total


def logit_part(probs, lidar, grad, mean):
    named = lidar[...]
    kept = (named >= 0).astype(jnp.float32)
    expected = mean[...]

    def one(depth, carry):
        prob = probs[pl.ds(depth, 1)][0]
        hit = (named == depth).astype(jnp.float32)
        value = prob * (grad[pl.ds(depth, 1)][0] - expected) + DEPTH_WEIGHT * (
            kept * prob - hit
        )
        grad[pl.ds(depth, 1)] = value[None]
        return carry

    lax.fori_loop(0, probs.shape[0], one, 0, unroll=2)


def sum_kernel(
    chips, terms, wide, probs, context, lidar, out, logit_grad, context_grad,
    features, mean, pair, local, stage_r, stage_l, land_r, land_l,
    pair_sems, ring_r, ring_l, pass_r, pass_l,
):
    me = lax.axis_index("blk")
    core = me % 2
    chip = me // 2
    blocks = 2 * chips
    partner = me + 1 - 2 * core
    right = (me + 2) % blocks
    left = (me + blocks - 2) % blocks
    rights = chips // 2
    lefts = chips - 1 - rights
    barrier = pltpu.get_barrier_semaphore()
    for other in (partner, right, left):
        greet(barrier, other)
    pl.semaphore_wait(barrier, 3)
    swap = remote(terms.at[1 - core], pair, pair_sems.at[0], pair_sems.at[1], partner)
    swap.start()
    features[...] = context[...].astype(jnp.float32)
    mean[...] = jnp.zeros_like(mean)
    parts = 2 * rights
    depths = probs.shape[0] // parts
    widths = context.shape[0] // parts
    swap.wait_recv()
    local[...] = (
        terms[pl.ds(core, 1)][0].astype(jnp.float32) + pair[...].astype(jnp.float32)
    )
    moves_r = []
    moves_l = []
    for step in range(rights):
        chunk = (chip + rights - step) % chips
        value = local[pl.ds(chunk, 1)][0]
        if step:
            moves_r[-1].wait_recv()
            value = value + land_r[step - 1].astype(jnp.float32)
        stage_r[step] = value.astype(stage_r.dtype)
        move = remote(
            stage_r.at[step], land_r.at[step], ring_r.at[0, step], ring_r.at[1, step], right
        )
        move.start()
        moves_r.append(move)
        if step < lefts:
            chunk = (chip + chips - lefts + step) % chips
            value = local[pl.ds(chunk, 1)][0]
            if step:
                moves_l[-1].wait_recv()
                value = value + land_l[step - 1].astype(jnp.float32)
            stage_l[step] = value.astype(stage_l.dtype)
            move = remote(
                stage_l.at[step], land_l.at[step], ring_l.at[0, step], ring_l.at[1, step], left
            )
            move.start()
            moves_l.append(move)
        for part in (2 * step, 2 * step + 1):
            context_part(wide, probs, context_grad, part * widths, widths)
    moves_l[-1].wait_recv()
    moves_r[-1].wait_recv()
    total = (
        local[pl.ds(chip, 1)][0]
        + land_r[rights - 1].astype(jnp.float32)
        + land_l[lefts - 1].astype(jnp.float32)
    )
    out[pl.ds(core, 1), pl.ds(chip, 1)] = total.astype(out.dtype)[None, None]

    def passing_r(step, origin):
        block = out.at[core, (origin + chips - step) % chips]
        return remote(block, block, pass_r.at[0, step], pass_r.at[1, step], right)

    def passing_l(step, origin):
        block = out.at[core, (origin + step) % chips]
        return remote(block, block, pass_l.at[0, step], pass_l.at[1, step], left)

    for step in range(rights):
        if step:
            passing_r(step - 1, chip + chips - 1).wait_recv()
        passing_r(step, chip).start()
        if step < lefts:
            if step:
                passing_l(step - 1, chip + 1).wait_recv()
            passing_l(step, chip).start()
        for part in (2 * step, 2 * step + 1):
            prob_part(wide, features, probs, logit_grad, mean, part * depths, depths)
    passing_l(lefts - 1, chip + 1).wait_recv()
    passing_r(rights - 1, chip + chips - 1).wait_recv()
    whole = remote(
        out.at[core], out.at[core], pair_sems.at[2], pair_sems.at[3], partner
    )
    whole.start()
    logit_part(probs, lidar, logit_grad, mean)
    remote(
        out.at[1 - core], out.at[1 - core], pair_sems.at[2], pair_sems.at[3], partner
    ).wait_recv()
    whole.wait_send()
    swap.wait_send()
    for move in moves_r + moves_l:
        move.wait_send()
    for step in range(rights):
        passing_r(step, chip).wait_send()
    for step in range(lefts):
        passing_l(step, chip).wait_send()


def slid(field, step):
    length = field.shape[0]
    moved = pltpu.roll(field, step % length, 0)
    row = lax.broadcasted_iota(jnp.int32, field.shape, 0)
    empty = 0 if step > 0 else length - 1
    return jnp.where(row == empty, 0.0, moved)


def back_taps(rows, weights):
    columns = []
    for tap_col in range(3):
        total = None
        for tap_row, row in enumerate(rows):
            term = lax.dot_general(
                row,
                weights(tap_row, tap_col),
                (((1,), (1,)), ((), ())),
                preferred_element_type=jnp.float32,
            )
            total = term if total is None else total + term
        columns.append(total)
    return columns[1] + slid(columns[0], -1) + slid(columns[2], 1)


def back_kernel(low, mid, high, hidden, weight2, weight1, pre, bev_grad, recent):
    step = pl.program_id(0)
    act_grad = back_taps(
        (high[0], mid[0], low[0]), lambda row, col: weight2[row, col]
    )
    value = (act_grad * silu_slope(hidden[0])).astype(pre.dtype)
    pre[0] = value
    recent[pl.ds(step % 3, 1)] = value[None]

    @pl.when(step >= 2)
    def _():
        rows = [recent[pl.ds((step + 3 - tap) % 3, 1)][0] for tap in range(3)]
        grad = back_taps(rows, lambda row, col: weight1[row, col])
        bev_grad[0] = grad[:, : bev_grad.shape[2]].astype(bev_grad.dtype)


def backward(upstream_wide, hidden_pre, conv2_weight, conv1_weight):
    height, length, width = hidden_pre.shape
    channels = conv1_weight.shape[2]
    weight1 = jnp.pad(conv1_weight, ((0, 0), (0, 0), (0, -channels % 128), (0, 0)))

    def line(offset):
        return pl.BlockSpec((1, length, width), lambda step: (step + offset, 0, 0))

    def whole(array):
        return pl.BlockSpec(array.shape, lambda step: (0,) * array.ndim)

    return pl.pallas_call(
        back_kernel,
        grid=(height,),
        out_shape=(
            jax.ShapeDtypeStruct((height, length, width), jnp.bfloat16),
            jax.ShapeDtypeStruct((height - 2, length, channels), jnp.bfloat16),
        ),
        in_specs=[
            line(0), line(1), line(2), line(0), whole(conv2_weight), whole(weight1)
        ],
        out_specs=(
            line(0),
            pl.BlockSpec((1, length, channels), lambda step: (jnp.maximum(step - 2, 0), 0, 0)),
        ),
        scratch_shapes=[pltpu.VMEM((3, length, width), jnp.bfloat16)],
        cost_estimate=pl.CostEstimate(
            flops=2 * 9 * height * length * width * (width + 128),
            bytes_accessed=16 * height * length * width,
            transcendentals=height * length * width,
        ),
        name="backward_convs",
    )(upstream_wide, upstream_wide, upstream_wide, hidden_pre, conv2_weight, weight1)


VMEM = pl.BlockSpec(memory_space=pltpu.VMEM)


def scatter_pieces(pieces, bands):
    blocks = lax.axis_size("blk")
    shape = pieces.shape[1:]

    def kernel(*refs):
        scatter_kernel(blocks, bands, *refs)

    return pl.pallas_call(
        kernel,
        out_shape=jax.ShapeDtypeStruct((2,) + shape, pieces.dtype),
        in_specs=[VMEM],
        out_specs=VMEM,
        scratch_shapes=[
            pltpu.VMEM((2 * bands,) + shape, pieces.dtype),
            pltpu.SemaphoreType.DMA((bands + 2,)),
            pltpu.SemaphoreType.DMA((2 * bands,)),
        ],
        compiler_params=pltpu.CompilerParams(collective_id=0, has_side_effects=True),
        name="scatter_pieces",
    )(pieces)


def gather_replies(replies, bands):
    blocks = lax.axis_size("blk")
    shape = replies.shape[1:]

    def kernel(*refs):
        reply_kernel(blocks, bands, *refs)

    return pl.pallas_call(
        kernel,
        out_shape=jax.ShapeDtypeStruct((bands + 2,) + shape, replies.dtype),
        in_specs=[VMEM],
        out_specs=VMEM,
        scratch_shapes=[
            pltpu.SemaphoreType.DMA((2 * bands,)),
            pltpu.SemaphoreType.DMA((bands + 2,)),
        ],
        compiler_params=pltpu.CompilerParams(collective_id=1, has_side_effects=True),
        name="gather_replies",
    )(replies)


def summed(terms, wide, probs, context, lidar):
    chips = terms.shape[1]
    rights = chips // 2
    lefts = chips - 1 - rights
    block = terms.shape[2:]
    kind = terms.dtype

    def kernel(*refs):
        sum_kernel(chips, *refs)

    return pl.pallas_call(
        kernel,
        out_shape=(
            jax.ShapeDtypeStruct(terms.shape, kind),
            jax.ShapeDtypeStruct(probs.shape, jnp.float32),
            jax.ShapeDtypeStruct(context.shape, context.dtype),
        ),
        in_specs=[VMEM] * 5,
        out_specs=(VMEM,) * 3,
        scratch_shapes=[
            pltpu.VMEM(context.shape, jnp.float32),
            pltpu.VMEM(probs.shape[1:], jnp.float32),
            pltpu.VMEM((chips,) + block, kind),
            pltpu.VMEM((chips,) + block, jnp.float32),
            pltpu.VMEM((rights,) + block, kind),
            pltpu.VMEM((lefts,) + block, kind),
            pltpu.VMEM((rights,) + block, kind),
            pltpu.VMEM((lefts,) + block, kind),
            pltpu.SemaphoreType.DMA((4,)),
            pltpu.SemaphoreType.DMA((2, rights)),
            pltpu.SemaphoreType.DMA((2, lefts)),
            pltpu.SemaphoreType.DMA((2, rights)),
            pltpu.SemaphoreType.DMA((2, lefts)),
        ],
        compiler_params=pltpu.CompilerParams(collective_id=2, has_side_effects=True),
        name="sum_gradients",
    )(terms, wide, probs, context, lidar)


def tripled(field):
    length = field.shape[1]
    padded = jnp.pad(field, ((0, 0), (1, 1), (0, 0)))
    return jnp.concatenate([padded[:, col : col + length] for col in range(3)], axis=2)


def conv_rows(triple, weight):
    height = triple.shape[0] - 2
    length = triple.shape[1]
    wide = jnp.concatenate([triple[row : row + height] for row in range(3)], axis=2)
    flat = wide.reshape(height * length, -1)
    return jnp.dot(
        flat, weight.reshape(-1, weight.shape[3]), preferred_element_type=jnp.float32
    ).reshape(height, length, weight.shape[3])


def weight_grad(triple, upstream):
    height, length, width = upstream.shape
    flat = upstream.reshape(height * length, width)
    rows = []
    for row in range(3):
        left = triple[row : row + height].reshape(height * length, -1)
        rows.append(
            lax.dot_general(
                left, flat, (((0,), (0,)), ((), ())), preferred_element_type=jnp.float32
            ).astype(jnp.bfloat16)
        )
    return jnp.concatenate(rows, axis=0)


def shards(
    depth_logits, context, lidar_bins, az_map, rng_map, conv1_weight, conv2_weight, out_grad
):
    blocks = lax.axis_size("blk")
    position = lax.axis_index("blk")
    cameras = az_map.shape[0]
    bands = blocks // cameras
    sector, length, hidden_width = out_grad.shape
    bin_count = depth_logits.shape[1]
    channels = context.shape[1]
    columns = depth_logits.shape[3]
    camera = position // bands
    band = position % bands
    upstream_wide = with_halo(out_grad, 2)
    depth_prob = jax.nn.softmax(depth_logits[0], axis=0)
    probs_low = depth_prob.astype(jnp.bfloat16)
    view_context = context[0]
    wedge = jnp.einsum("brc,hrc->cbh", probs_low, view_context, preferred_element_type=jnp.float32)
    wedge = wedge.astype(jnp.bfloat16).reshape(columns, bin_count * channels)
    az_row = lax.dynamic_slice_in_dim(az_map, camera, 1, 0)[0]
    span = (bands + 2) * sector
    seen = ((camera * bands + blocks - 1) * sector + jnp.arange(span, dtype=jnp.int32)) % (
        blocks * sector
    )
    column_hot = (seen[:, None] == az_row[None, :]).astype(jnp.bfloat16)
    pieces = jnp.dot(column_hot, wedge, preferred_element_type=jnp.float32).astype(jnp.bfloat16)
    sums = scatter_pieces(pieces.reshape(bands + 2, sector, bin_count * channels), bands)
    neighbour = jnp.where(band == 0, camera + cameras - 1, camera + 1) % cameras
    cells = jnp.arange(length, dtype=jnp.int32)
    ranges = jnp.concatenate(
        [
            lax.dynamic_slice_in_dim(rng_map, camera, 1, 0),
            lax.dynamic_slice_in_dim(rng_map, neighbour, 1, 0),
        ],
        axis=0,
    )
    range_hot = (ranges[:, None, :] == cells[None, :, None]).astype(jnp.bfloat16)
    bev = jnp.einsum(
        "nrb,nabh->arh",
        range_hot,
        sums.reshape(2, sector, bin_count, channels),
        preferred_element_type=jnp.float32,
    ).astype(jnp.bfloat16)
    bev_triple = tripled(with_halo(bev, 2))
    hidden_pre = conv_rows(bev_triple, conv1_weight)
    activated = jax.nn.silu(hidden_pre).astype(jnp.bfloat16)
    conv2_grad = weight_grad(tripled(activated), out_grad)
    pre_grad, bev_grad = backward(upstream_wide, hidden_pre, conv2_weight, conv1_weight)
    conv1_grad = weight_grad(bev_triple[1:-1], pre_grad[1:-1])
    replies = jnp.einsum(
        "nrb,arh->nabh", range_hot, bev_grad, preferred_element_type=jnp.float32
    ).astype(jnp.bfloat16)
    gathered = gather_replies(replies.reshape(2, sector, bin_count * channels), bands)
    wide = lax.dot_general(
        gathered.reshape(span, bin_count * channels),
        column_hot,
        (((0,), (0,)), ((), ())),
        preferred_element_type=jnp.float32,
    )
    rows1 = conv1_grad.shape[0]
    rows2 = conv2_grad.shape[0]
    step = 16 * blocks
    padding = -(rows1 + rows2) % step
    terms = jnp.concatenate(
        [conv1_grad, conv2_grad, jnp.zeros((padding, hidden_width), jnp.bfloat16)], axis=0
    )
    terms, logit_grad, context_grad = summed(
        terms.reshape(2, blocks // 2, -1, hidden_width),
        wide,
        depth_prob,
        view_context,
        lidar_bins[0],
    )
    terms = terms.reshape(-1, hidden_width).astype(jnp.float32)
    return (
        logit_grad[None],
        context_grad[None],
        terms[:rows1].reshape(3, 3, channels, hidden_width),
        terms[rows1 : rows1 + rows2].reshape(3, 3, hidden_width, hidden_width),
    )


def solution(mesh):
    return jax.shard_map(
        shards,
        mesh=mesh,
        in_specs=(
            P(("group", "blk"), None, None, None),
            P(("group", "blk"), None, None, None),
            P(("group", "blk"), None, None),
            P(),
            P(),
            P(),
            P(),
            P(("group", "blk"), None, None),
        ),
        out_specs=(
            P(("group", "blk"), None, None, None),
            P(("group", "blk"), None, None, None),
            P("group", None, None, None),
            P("group", None, None, None),
        ),
        check_vma=False,
    )
```

```python
import jax
import jax.numpy as jnp
from jax import lax
from jax.experimental import pallas as pl
from jax.experimental.pallas import tpu as pltpu
from jax.sharding import PartitionSpec as P

DEPTH_WEIGHT = 3.0


def with_halo(cells, width):
    count = lax.axis_size("blk")
    head = cells[:width]
    tail = cells[cells.shape[0] - width :]
    return jnp.concatenate(
        [
            lax.ppermute(tail, "blk", [(i, (i + 1) % count) for i in range(count)]),
            cells,
            lax.ppermute(head, "blk", [((i + 1) % count, i) for i in range(count)]),
        ],
        axis=0,
    )


def silu_slope(value):
    logistic = jax.nn.sigmoid(value)
    return logistic * (1.0 + value * (1.0 - logistic))


def remote(src, dst, send_sem, recv_sem, target):
    return pltpu.make_async_remote_copy(
        src_ref=src,
        dst_ref=dst,
        send_sem=send_sem,
        recv_sem=recv_sem,
        device_id={"blk": target},
        device_id_type=pl.DeviceIdType.MESH,
    )


def greet(semaphore, target):
    pl.semaphore_signal(
        semaphore,
        inc=1,
        device_id={"blk": target},
        device_id_type=pl.DeviceIdType.MESH,
    )


def scatter_kernel(blocks, bands, pieces, sums, slots, send_sems, recv_sems):
    me = lax.axis_index("blk")
    band = me % bands
    first = me - band
    before = (first + blocks - bands) % blocks
    after = (first + bands) % blocks
    barrier = pltpu.get_barrier_semaphore()
    for other in range(bands):
        @pl.when(band != other)
        def _():
            greet(barrier, first + other)

        @pl.when(band == 0)
        def _():
            greet(barrier, before + other)

        @pl.when(band == bands - 1)
        def _():
            greet(barrier, after + other)
    pl.semaphore_wait(barrier, bands + 1)

    def outgoing(part):
        near = 1 <= part <= bands
        slot = band if near else bands + band
        target = (first + blocks - 1 + part) % blocks
        return remote(
            pieces.at[part], slots.at[slot], send_sems.at[part], recv_sems.at[slot], target
        )

    def arriving(slot):
        return remote(pieces.at[0], slots.at[slot], send_sems.at[0], recv_sems.at[slot], first)

    for part in (0, bands + 1):
        outgoing(part).start()
    for part in range(1, bands + 1):
        @pl.when(band != part - 1)
        def _():
            outgoing(part).start()
    slots[pl.ds(band, 1)] = pieces[pl.ds(band + 1, 1)]
    for slot in range(bands):
        @pl.when(band != slot)
        def _():
            arriving(slot).wait_recv()
    total = slots[0].astype(jnp.float32)
    for slot in range(1, bands):
        total = total + slots[slot].astype(jnp.float32)
    sums[0] = total.astype(sums.dtype)
    edge = jnp.logical_or(band == 0, band == bands - 1)

    @pl.when(edge)
    def _():
        for slot in range(bands, 2 * bands):
            arriving(slot).wait_recv()
        side = slots[bands].astype(jnp.float32)
        for slot in range(bands + 1, 2 * bands):
            side = side + slots[slot].astype(jnp.float32)
        sums[1] = side.astype(sums.dtype)

    @pl.when(jnp.logical_not(edge))
    def _():
        sums[1] = jnp.zeros(sums.shape[1:], sums.dtype)

    for part in (0, bands + 1):
        outgoing(part).wait_send()
    for part in range(1, bands + 1):
        @pl.when(band != part - 1)
        def _():
            outgoing(part).wait_send()


def reply_kernel(blocks, bands, replies, gathered, send_sems, recv_sems, hand_sems):
    me = lax.axis_index("blk")
    band = me % bands
    core = me % 2
    first = me - band
    partner = me + 1 - 2 * core
    before = (first + blocks - bands) % blocks
    after = (first + bands) % blocks
    edge = jnp.logical_or(band == 0, band == bands - 1)
    own = band + 1
    order = list(range(1, bands + 1)) + [0, bands + 1]
    barrier = pltpu.get_barrier_semaphore()
    greet(barrier, partner)
    for part in order:
        @pl.when(jnp.logical_and((part + 1) % 2 == core, part != own))
        def _():
            greet(barrier, (first + blocks - 1 + part) % blocks)

    @pl.when(edge)
    def _():
        pl.semaphore_wait(barrier, bands)

    @pl.when(jnp.logical_not(edge))
    def _():
        pl.semaphore_wait(barrier, bands // 2)

    def move(source, part, sem, target):
        return remote(
            replies.at[source], gathered.at[part], send_sems.at[sem], recv_sems.at[part], target
        )

    def sends(action):
        for other in range(bands):
            alike = other % 2 == core

            @pl.when(jnp.logical_and(alike, band != other))
            def _():
                action(move(0, own, other, first + other))

            @pl.when(jnp.logical_and(alike, band == 0))
            def _():
                action(move(1, bands + 1, bands + other, before + other))

            @pl.when(jnp.logical_and(alike, band == bands - 1))
            def _():
                action(move(1, 0, bands + other, after + other))

    def handing(part):
        block = gathered.at[part]
        return remote(block, block, hand_sems.at[part], recv_sems.at[part], partner)

    def arriving(part):
        return remote(
            replies.at[0], gathered.at[part], send_sems.at[0], recv_sems.at[part], partner
        )

    given = remote(
        replies.at[0], gathered.at[own], hand_sems.at[own], recv_sems.at[own], partner
    )
    sends(lambda copy: copy.start())
    given.start()
    gathered[pl.ds(own, 1)] = replies[pl.ds(0, 1)]
    for part in order:
        @pl.when(jnp.logical_and((part + 1) % 2 == core, part != own))
        def _():
            arriving(part).wait_recv()
            handing(part).start()
    for part in order:
        @pl.when((part + 1) % 2 != core)
        def _():
            arriving(part).wait_recv()

        @pl.when(jnp.logical_and((part + 1) % 2 == core, part != own))
        def _():
            handing(part).wait_send()
    given.wait_send()
    sends(lambda copy: copy.wait_send())


def context_part(wide, probs, grad, start, count):
    channels = grad.shape[0]

    def add(depth, sums):
        weight = probs[pl.ds(depth, 1)][0]
        return tuple(
            held + wide[pl.ds(depth * channels + start + step, 1), :] * weight
            for step, held in enumerate(sums)
        )

    zero = jnp.zeros(probs.shape[1:], jnp.float32)
    sums = lax.fori_loop(0, probs.shape[0], add, (zero,) * count, unroll=2)
    for step, held in enumerate(sums):
        grad[start + step] = held.astype(grad.dtype)


def prob_part(wide, features, probs, grad, mean, start, count):
    channels = features.shape[0]

    def add(channel, sums):
        feature = features[pl.ds(channel, 1)][0]
        return tuple(
            held + wide[pl.ds((start + step) * channels + channel, 1), :] * feature
            for step, held in enumerate(sums)
        )

    zero = jnp.zeros(probs.shape[1:], jnp.float32)
    sums = lax.fori_loop(0, channels, add, (zero,) * count, unroll=2)
    total = mean[...]
    for step, held in enumerate(sums):
        grad[start + step] = held
        total = total + probs[start + step] * held
    mean[...] = total


def logit_part(probs, lidar, grad, mean):
    named = lidar[...]
    kept = (named >= 0).astype(jnp.float32)
    expected = mean[...]

    def one(depth, carry):
        prob = probs[pl.ds(depth, 1)][0]
        hit = (named == depth).astype(jnp.float32)
        value = prob * (grad[pl.ds(depth, 1)][0] - expected) + DEPTH_WEIGHT * (
            kept * prob - hit
        )
        grad[pl.ds(depth, 1)] = value[None]
        return carry

    lax.fori_loop(0, probs.shape[0], one, 0, unroll=2)


def sum_kernel(
    chips, terms, wide, probs, context, lidar, first_grad, second_grad, logit_grad,
    context_grad, features, mean, pair, local, out, chain_from, own_from, chain_to, own_to,
    pair_sems, chain_sems, own_sems, near_sems, far_sems,
):
    me = lax.axis_index("blk")
    core = me % 2
    chip = me // 2
    blocks = 2 * chips
    partner = me + 1 - 2 * core
    ways = ((0, 1, chips // 2), (1, -1, chips - 1 - chips // 2))
    rounds = chips // 4
    kind = terms.dtype

    def place(step):
        return (chip + step + chips) % chips

    def device(step):
        return (me + 2 * step + blocks) % blocks

    barrier = pltpu.get_barrier_semaphore()
    for other in (partner, device(1), device(-1), device(2), device(-2)):
        greet(barrier, other)
    pl.semaphore_wait(barrier, 5)
    swap = remote(terms.at[1 - core], pair, pair_sems.at[0], pair_sems.at[1], partner)
    swap.start()
    features[...] = context[...].astype(jnp.float32)
    mean[...] = jnp.zeros_like(mean)
    parts = 4 * rounds
    depths = probs.shape[0] // parts
    widths = context.shape[0] // parts
    swap.wait_recv()
    local[...] = (
        terms[pl.ds(core, 1)][0].astype(jnp.float32) + pair[...].astype(jnp.float32)
    )

    def mine(step):
        return local[pl.ds(place(step), 1)][0]

    def chain_move(way, sign, reach, index):
        hop = 2 if reach - 2 * index >= 2 else 1
        return remote(
            chain_from.at[way, index], chain_to.at[way, index],
            chain_sems.at[way, 0, index], chain_sems.at[way, 1, index], device(sign * hop),
        )

    def own_move(way, sign, index):
        return remote(
            own_from.at[way, index], own_to.at[way, index],
            own_sems.at[way, 0, index], own_sems.at[way, 1, index], device(sign),
        )

    for index in range(rounds):
        for way, sign, reach in ways:
            value = mine(sign * (reach - 2 * index))
            if index:
                chain_move(way, sign, reach, index - 1).wait_recv()
                own_move(way, sign, index - 1).wait_recv()
                value = value + chain_to[way, index - 1].astype(jnp.float32)
                value = value + own_to[way, index - 1].astype(jnp.float32)
            chain_from[way, index] = value.astype(kind)
            chain_move(way, sign, reach, index).start()
        for way, sign, reach in ways:
            if index < reach // 2:
                own_from[way, index] = mine(sign * (reach - 1 - 2 * index)).astype(kind)
                own_move(way, sign, index).start()
        for part in range(4 * index, 4 * index + 4):
            context_part(wide, probs, context_grad, part * widths, widths)
    total = mine(0)
    for way, sign, reach in ways:
        chain_move(way, sign, reach, rounds - 1).wait_recv()
        total = total + chain_to[way, rounds - 1].astype(jnp.float32)
        if rounds == reach // 2:
            own_move(way, sign, rounds - 1).wait_recv()
            total = total + own_to[way, rounds - 1].astype(jnp.float32)
    out[pl.ds(core, 1), pl.ds(chip, 1)] = total.astype(kind)[None, None]

    def passing(way, sign, index, hop, origin):
        block = out.at[core, (chip + origin - 2 * sign * index + 2 * chips) % chips]
        sems = near_sems if hop == 1 else far_sems
        return remote(
            block, block, sems.at[way, 0, index], sems.at[way, 1, index], device(sign * hop)
        )

    def hops(reach, index):
        return [hop for hop in (2, 1) if 2 * index + hop <= reach]

    for index in range(rounds):
        for way, sign, reach in ways:
            if index:
                passing(way, sign, index - 1, 2, -2 * sign).wait_recv()
            for hop in hops(reach, index):
                passing(way, sign, index, hop, 0).start()
        for part in range(4 * index, 4 * index + 4):
            prob_part(wide, features, probs, logit_grad, mean, part * depths, depths)
    for way, sign, reach in ways:
        for index in range(rounds):
            passing(way, sign, index, 1, -sign).wait_recv()
        if 2 in hops(reach, rounds - 1):
            passing(way, sign, rounds - 1, 2, -2 * sign).wait_recv()
    whole = remote(
        out.at[core], out.at[core], pair_sems.at[2], pair_sems.at[3], partner
    )
    whole.start()
    logit_part(probs, lidar, logit_grad, mean)
    remote(
        out.at[1 - core], out.at[1 - core], pair_sems.at[2], pair_sems.at[3], partner
    ).wait_recv()
    height = terms.shape[2]
    split = first_grad.shape[0]
    final = split + second_grad.shape[0]
    for half in range(2):
        for chunk in range(chips):
            low = (half * chips + chunk) * height
            block = out[half, chunk].astype(jnp.float32)
            cut = min(max(split - low, 0), height)
            end = min(final - low, height)
            if cut > 0:
                first_grad[low : low + cut] = block[:cut]
            if end > cut:
                second_grad[low + cut - split : low + end - split] = block[cut:end]
    whole.wait_send()
    swap.wait_send()
    for way, sign, reach in ways:
        for index in range(rounds):
            chain_move(way, sign, reach, index).wait_send()
            if index < reach // 2:
                own_move(way, sign, index).wait_send()
            for hop in hops(reach, index):
                passing(way, sign, index, hop, 0).wait_send()


def slid(field, step):
    length = field.shape[0]
    moved = pltpu.roll(field, step % length, 0)
    row = lax.broadcasted_iota(jnp.int32, field.shape, 0)
    empty = 0 if step > 0 else length - 1
    return jnp.where(row == empty, 0.0, moved)


def back_taps(rows, weights):
    columns = []
    for tap_col in range(3):
        total = None
        for tap_row, row in enumerate(rows):
            term = lax.dot_general(
                row,
                weights(tap_row, tap_col),
                (((1,), (1,)), ((), ())),
                preferred_element_type=jnp.float32,
            )
            total = term if total is None else total + term
        columns.append(total)
    return columns[1] + slid(columns[0], -1) + slid(columns[2], 1)


def back_kernel(low, mid, high, hidden, weight2, weight1, pre, bev_grad, recent):
    step = pl.program_id(0)
    act_grad = back_taps(
        (high[0], mid[0], low[0]), lambda row, col: weight2[row, col]
    )
    value = (act_grad * silu_slope(hidden[0])).astype(pre.dtype)
    pre[0] = value
    recent[pl.ds(step % 3, 1)] = value[None]

    @pl.when(step >= 2)
    def _():
        rows = [recent[pl.ds((step + 3 - tap) % 3, 1)][0] for tap in range(3)]
        grad = back_taps(rows, lambda row, col: weight1[row, col])
        bev_grad[0] = grad[:, : bev_grad.shape[2]].astype(bev_grad.dtype)


def backward(upstream_wide, hidden_pre, conv2_weight, conv1_weight):
    height, length, width = hidden_pre.shape
    channels = conv1_weight.shape[2]
    weight1 = jnp.pad(conv1_weight, ((0, 0), (0, 0), (0, -channels % 128), (0, 0)))

    def line(offset):
        return pl.BlockSpec((1, length, width), lambda step: (step + offset, 0, 0))

    def whole(array):
        return pl.BlockSpec(array.shape, lambda step: (0,) * array.ndim)

    return pl.pallas_call(
        back_kernel,
        grid=(height,),
        out_shape=(
            jax.ShapeDtypeStruct((height, length, width), jnp.bfloat16),
            jax.ShapeDtypeStruct((height - 2, length, channels), jnp.bfloat16),
        ),
        in_specs=[
            line(0), line(1), line(2), line(0), whole(conv2_weight), whole(weight1)
        ],
        out_specs=(
            line(0),
            pl.BlockSpec((1, length, channels), lambda step: (jnp.maximum(step - 2, 0), 0, 0)),
        ),
        scratch_shapes=[pltpu.VMEM((3, length, width), jnp.bfloat16)],
        cost_estimate=pl.CostEstimate(
            flops=2 * 9 * height * length * width * (width + 128),
            bytes_accessed=16 * height * length * width,
            transcendentals=height * length * width,
        ),
        name="backward_convs",
    )(upstream_wide, upstream_wide, upstream_wide, hidden_pre, conv2_weight, weight1)


VMEM = pl.BlockSpec(memory_space=pltpu.VMEM)


def scatter_pieces(pieces, bands):
    blocks = lax.axis_size("blk")
    shape = pieces.shape[1:]

    def kernel(*refs):
        scatter_kernel(blocks, bands, *refs)

    return pl.pallas_call(
        kernel,
        out_shape=jax.ShapeDtypeStruct((2,) + shape, pieces.dtype),
        in_specs=[VMEM],
        out_specs=VMEM,
        scratch_shapes=[
            pltpu.VMEM((2 * bands,) + shape, pieces.dtype),
            pltpu.SemaphoreType.DMA((bands + 2,)),
            pltpu.SemaphoreType.DMA((2 * bands,)),
        ],
        compiler_params=pltpu.CompilerParams(collective_id=0, has_side_effects=True),
        name="scatter_pieces",
    )(pieces)


def gather_replies(replies, bands):
    blocks = lax.axis_size("blk")
    shape = replies.shape[1:]

    def kernel(*refs):
        reply_kernel(blocks, bands, *refs)

    return pl.pallas_call(
        kernel,
        out_shape=jax.ShapeDtypeStruct((bands + 2,) + shape, replies.dtype),
        in_specs=[VMEM],
        out_specs=VMEM,
        scratch_shapes=[
            pltpu.SemaphoreType.DMA((2 * bands,)),
            pltpu.SemaphoreType.DMA((bands + 2,)),
            pltpu.SemaphoreType.DMA((bands + 2,)),
        ],
        compiler_params=pltpu.CompilerParams(collective_id=1, has_side_effects=True),
        name="gather_replies",
    )(replies)


def summed(terms, wide, probs, context, lidar, rows1, rows2):
    chips = terms.shape[1]
    rounds = chips // 4
    block = terms.shape[2:]
    kind = terms.dtype

    def kernel(*refs):
        sum_kernel(chips, *refs)

    return pl.pallas_call(
        kernel,
        out_shape=(
            jax.ShapeDtypeStruct((rows1,) + block[1:], jnp.float32),
            jax.ShapeDtypeStruct((rows2,) + block[1:], jnp.float32),
            jax.ShapeDtypeStruct(probs.shape, jnp.float32),
            jax.ShapeDtypeStruct(context.shape, context.dtype),
        ),
        in_specs=[VMEM] * 5,
        out_specs=(VMEM,) * 4,
        scratch_shapes=[
            pltpu.VMEM(context.shape, jnp.float32),
            pltpu.VMEM(probs.shape[1:], jnp.float32),
            pltpu.VMEM((chips,) + block, kind),
            pltpu.VMEM((chips,) + block, jnp.float32),
            pltpu.VMEM((2, chips) + block, kind),
        ]
        + [pltpu.VMEM((2, rounds) + block, kind)] * 4
        + [pltpu.SemaphoreType.DMA((4,))]
        + [pltpu.SemaphoreType.DMA((2, 2, rounds))] * 4,
        compiler_params=pltpu.CompilerParams(collective_id=2, has_side_effects=True),
        name="sum_gradients",
    )(terms, wide, probs, context, lidar)


def tripled(field):
    length = field.shape[1]
    padded = jnp.pad(field, ((0, 0), (1, 1), (0, 0)))
    return jnp.concatenate([padded[:, col : col + length] for col in range(3)], axis=2)


def conv_rows(triple, weight):
    height = triple.shape[0] - 2
    length = triple.shape[1]
    wide = jnp.concatenate([triple[row : row + height] for row in range(3)], axis=2)
    flat = wide.reshape(height * length, -1)
    return jnp.dot(
        flat, weight.reshape(-1, weight.shape[3]), preferred_element_type=jnp.float32
    ).reshape(height, length, weight.shape[3])


def weight_grad(triple, upstream):
    height, length, width = upstream.shape
    flat = upstream.reshape(height * length, width)
    rows = []
    for row in range(3):
        left = triple[row : row + height].reshape(height * length, -1)
        rows.append(
            lax.dot_general(
                left, flat, (((0,), (0,)), ((), ())), preferred_element_type=jnp.float32
            ).astype(jnp.bfloat16)
        )
    return jnp.concatenate(rows, axis=0)


def shards(
    depth_logits, context, lidar_bins, az_map, rng_map, conv1_weight, conv2_weight, out_grad
):
    blocks = lax.axis_size("blk")
    position = lax.axis_index("blk")
    cameras = az_map.shape[0]
    bands = blocks // cameras
    sector, length, hidden_width = out_grad.shape
    bin_count = depth_logits.shape[1]
    channels = context.shape[1]
    columns = depth_logits.shape[3]
    camera = position // bands
    band = position % bands
    upstream_wide = with_halo(out_grad, 2)
    depth_prob = jax.nn.softmax(depth_logits[0], axis=0)
    probs_low = depth_prob.astype(jnp.bfloat16)
    view_context = context[0]
    wedge = jnp.einsum("brc,hrc->cbh", probs_low, view_context, preferred_element_type=jnp.float32)
    wedge = wedge.astype(jnp.bfloat16).reshape(columns, bin_count * channels)
    az_row = lax.dynamic_slice_in_dim(az_map, camera, 1, 0)[0]
    span = (bands + 2) * sector
    seen = ((camera * bands + blocks - 1) * sector + jnp.arange(span, dtype=jnp.int32)) % (
        blocks * sector
    )
    column_hot = (seen[:, None] == az_row[None, :]).astype(jnp.bfloat16)
    pieces = jnp.dot(column_hot, wedge, preferred_element_type=jnp.float32).astype(jnp.bfloat16)
    sums = scatter_pieces(pieces.reshape(bands + 2, sector, bin_count * channels), bands)
    neighbour = jnp.where(band == 0, camera + cameras - 1, camera + 1) % cameras
    cells = jnp.arange(length, dtype=jnp.int32)
    ranges = jnp.concatenate(
        [
            lax.dynamic_slice_in_dim(rng_map, camera, 1, 0),
            lax.dynamic_slice_in_dim(rng_map, neighbour, 1, 0),
        ],
        axis=0,
    )
    range_hot = (ranges[:, None, :] == cells[None, :, None]).astype(jnp.bfloat16)
    bev = jnp.einsum(
        "nrb,nabh->arh",
        range_hot,
        sums.reshape(2, sector, bin_count, channels),
        preferred_element_type=jnp.float32,
    ).astype(jnp.bfloat16)
    bev_triple = tripled(with_halo(bev, 2))
    hidden_pre = conv_rows(bev_triple, conv1_weight)
    activated = jax.nn.silu(hidden_pre).astype(jnp.bfloat16)
    conv2_grad = weight_grad(tripled(activated), out_grad)
    pre_grad, bev_grad = backward(upstream_wide, hidden_pre, conv2_weight, conv1_weight)
    conv1_grad = weight_grad(bev_triple[1:-1], pre_grad[1:-1])
    replies = jnp.einsum(
        "nrb,arh->nabh", range_hot, bev_grad, preferred_element_type=jnp.float32
    ).astype(jnp.bfloat16)
    gathered = gather_replies(replies.reshape(2, sector, bin_count * channels), bands)
    wide = lax.dot_general(
        gathered.reshape(span, bin_count * channels),
        column_hot,
        (((0,), (0,)), ((), ())),
        preferred_element_type=jnp.float32,
    )
    rows1 = conv1_grad.shape[0]
    rows2 = conv2_grad.shape[0]
    step = 16 * blocks
    padding = -(rows1 + rows2) % step
    terms = jnp.concatenate(
        [conv1_grad, conv2_grad, jnp.zeros((padding, hidden_width), jnp.bfloat16)], axis=0
    )
    first_grad, second_grad, logit_grad, context_grad = summed(
        terms.reshape(2, blocks // 2, -1, hidden_width),
        wide,
        depth_prob,
        view_context,
        lidar_bins[0],
        rows1,
        rows2,
    )
    return (
        logit_grad[None],
        context_grad[None],
        first_grad.reshape(3, 3, channels, hidden_width),
        second_grad.reshape(3, 3, hidden_width, hidden_width),
    )


def solution(mesh):
    return jax.shard_map(
        shards,
        mesh=mesh,
        in_specs=(
            P(("group", "blk"), None, None, None),
            P(("group", "blk"), None, None, None),
            P(("group", "blk"), None, None),
            P(),
            P(),
            P(),
            P(),
            P(("group", "blk"), None, None),
        ),
        out_specs=(
            P(("group", "blk"), None, None, None),
            P(("group", "blk"), None, None, None),
            P("group", None, None, None),
            P("group", None, None, None),
        ),
        check_vma=False,
    )
```
